768 devices in a mesh: lat: 48 (over z_lo, y, core), lon: 16 (over x, z_hi).
Axes of the slice: x: 4, y: 8, z: 12 (z_hi: 4, z_lo: 3; z = z_hi * 3 + z_lo), core: 2. Of those that a mesh axis runs over, the one named last changes fastest.
Arguments:
- fields: float32 [4, 6, 1536, 5120], P(None, None, 'lat', 'lon'), may hold values from -6 to 6
- dep_row: int32 [6, 1536, 5120], P(None, 'lat', 'lon'), may hold values from -4 to 1535, as said below
- dep_col: int32 [6, 1536, 5120], P(None, 'lat', 'lon'), may hold values from 0 to 5119, as said below
- weights: float32 [8, 6, 1536, 5120], P(None, None, 'lat', 'lon'), may hold values from -0.25 to 0.75
Outputs:
- departed: float32 [4, 6, 1536, 5120], P(None, None, 'lat', 'lon')
The draws below stay inside these ranges and needn't reach their ends.
Inputs may be any that keep to these rules, and one draw needn't show every extreme that they name: dep_row[l, i, j] lies within i - 4 to i. dep_col[l, i, j] equals (j + k) modulo 5120 for some k from -4 to 0.
All inputs are finite; a program needn't handle non-finite values.
Results may differ from the reference program's by a relative error of at most 0.0003.
Values sent between devices are 32-bit elements; how exact they have to be, the bound alone decides.
A program may use at most 32 MiB of HBM per device.

```python
import jax
import jax.numpy as jnp
from jax import lax

LEV = 6
FIELDS = 4
HALO = 4
NR = 1536
NC = 5120


def departures(key):
    base_key = jax.random.fold_in(key, 7713)
    key_rows, key_cols = jax.random.split(base_key)
    shape = (LEV, NR, NC)
    shift_rows = jax.random.randint(key_rows, shape, -3, 2, dtype=jnp.int32)
    shift_cols = jax.random.randint(key_cols, shape, -3, 2, dtype=jnp.int32)
    row_index = lax_iota(shape, 1)
    col_index = lax_iota(shape, 2)
    rows = row_index + shift_rows - 1
    cols = jnp.mod(col_index + shift_cols - 1, NC)
    return (rows.astype(jnp.int32), cols.astype(jnp.int32))


def lax_iota(shape, dim):
    return jax.lax.broadcasted_iota(jnp.int32, shape, dim)


def draw_dep_row(key, part):
    return departures(key)[0]


def draw_dep_col(key, part):
    return departures(key)[1]


def block_levels(stream_key, dims, cuts, least, top_value):
    gain, own = 1.0, jax.random.fold_in(stream_key, 6)
    for dim, blocks in cuts:
        steps = jnp.exp(jax.random.uniform(jax.random.fold_in(own, dim), (blocks,), jnp.float32, least / len(cuts), top_value / len(cuts)))
        gain = gain * jnp.repeat(steps, dims[dim] // blocks).reshape([-1 if axis == dim else 1 for axis in range(len(dims))])
    return gain


def bell_draw(own_key, extent, deviation, most, pieces=(), held_as=jnp.bfloat16):
    drawn = deviation * jax.random.normal(own_key, extent, jnp.float32)
    if pieces:
        drawn = drawn * block_levels(own_key, extent, pieces, -0.22, 0.18)
    return jnp.clip(drawn, -most, most).astype(held_as)


def setup_inputs(seed: int = 0) -> dict:
    key_of = jax.random.split(jax.random.key(seed), 5)
    return {
        "fields": bell_draw(key_of[0], (FIELDS, LEV, NR, NC), 1.0, 6.0, ((2, 48), (3, 16)), jnp.float32),
        "dep_row": draw_dep_row(jax.random.fold_in(key_of[4], 71), 0),
        "dep_col": draw_dep_col(jax.random.fold_in(key_of[4], 71), 0),
        "weights": jnp.clip(-0.25 + 1.0 * jax.random.uniform(key_of[3], (8, LEV, NR, NC), jnp.float32) ** block_levels(key_of[3], (8, LEV, NR, NC), ((2, 48), (3, 16)), -0.2, 0.2), -0.25, 0.75),
    }


def interpolate_level(item):
    field, rows, cols, weight = item
    half = NC // 2
    north = jnp.roll(field[:, :HALO][:, ::-1], half, axis=2)
    south = jnp.roll(field[:, NR - HALO:][:, ::-1], half, axis=2)
    tall = jnp.concatenate([north, field, south], axis=1)
    padded = jnp.concatenate([tall[:, :, NC - HALO:], tall, tall[:, :, :HALO]], axis=2)
    width = NC + 2 * HALO
    flat = padded.reshape(FIELDS, -1)
    base = ((rows + HALO) * width + (cols + HALO)).astype(jnp.int32).reshape(-1)
    total = jnp.zeros((FIELDS, NR * NC), jnp.float32)
    for first in range(4):
        line = jnp.zeros((FIELDS, NR * NC), jnp.float32)
        for second in range(4):
            values = jnp.take(flat, base + first * width + second, axis=1)
            line = line + weight[4 + second].reshape(1, -1) * values
        total = total + weight[first].reshape(1, -1) * line
    return total.reshape(FIELDS, NR, NC)


def reference(fields, dep_row, dep_col, weights):
    result = lax.map(interpolate_level, (jnp.transpose(fields, (1, 0, 2, 3)), dep_row, dep_col, jnp.transpose(weights, (1, 0, 2, 3))))
    return jnp.transpose(result, (1, 0, 2, 3))
```

```python
import functools

import jax
import jax.numpy as jnp
from jax import lax
from jax.experimental import pallas as pl
from jax.experimental.pallas import tpu as pltpu
from jax.sharding import PartitionSpec as P

MESH = pl.DeviceIdType.MESH
F32 = jnp.float32
LANES = 128
SUB = 8
HALO = 4
SPAN = 2 * HALO
EARLY_EVERY = 4


def lane_iota(shape):
    return lax.broadcasted_iota(jnp.int32, shape, len(shape) - 1)


def sub_iota(shape):
    return lax.broadcasted_iota(jnp.int32, shape, len(shape) - 2)


def roll(x, shift, axis):
    size = x.shape[axis]
    return pltpu.roll(x, shift % size, axis) if shift % size else x


def widen(x):
    width = x.shape[-1]
    if width == LANES:
        return x
    return jnp.concatenate([x, jnp.zeros(x.shape[:-1] + (LANES - width,), x.dtype)], axis=-1)


def neighbours(band, sector, nband, nsector):
    east = lax.rem(sector + 1, nsector)
    west = lax.rem(sector + nsector - 1, nsector)
    top, bottom = band == 0, band == nband - 1
    north, south = jnp.where(top, band, band - 1), jnp.where(bottom, band, band + 1)
    half = nsector // 2
    turn_n, turn_s = jnp.where(top, half, 0), jnp.where(bottom, half, 0)

    def at(row, col, turn):
        return (row, lax.rem(col + turn, nsector))

    return {
        "E": (band, east), "W": (band, west),
        "N": at(north, sector, turn_n), "S": at(south, sector, turn_s),
        "NE": at(north, east, turn_n), "NW": at(north, west, turn_n),
        "SE": at(south, east, turn_s), "SW": at(south, west, turn_s),
    }


def select_weights(offset, taps):
    masks = [offset == o for o in range(HALO + 1)]
    out = []
    for s in range(SPAN):
        term = jnp.zeros(offset.shape, F32)
        for a in range(4):
            if 0 <= s - a <= HALO:
                term = jnp.where(masks[s - a], taps[a], term)
        out.append(term)
    return out


def flip4(x):
    i = sub_iota(x.shape)
    x = jnp.where((i & 1) == 1, roll(x, 1, 0), roll(x, -1, 0))
    return jnp.where((i & 2) == 2, roll(x, 2, 0), roll(x, -2, 0))


def kernel(dims, fields, dep_row, dep_col, weights, out,
           fv, drv, dcv, wv, ov, rc, sh, slab, slab_in, strip, strip_in, corner, corner_in,
           tn, xx, pw, pd, in_sem, out_sem, send_sem, recv_sem):
    nf, nl, rows, cols, nband, nsector, total_cols = dims
    band, sector = lax.axis_index("lat"), lax.axis_index("lon")
    there = neighbours(band, sector, nband, nsector)
    top, bottom = band == 0, band == nband - 1
    tiles = pl.cdiv(cols, LANES)
    tail = cols - (tiles - 1) * LANES
    widths = [LANES] * (tiles - 1) + [tail]
    blocks = rows // SUB
    last = rows - SUB
    lane = lane_iota((SUB, LANES))
    sub = sub_iota((SUB, LANES))

    loads = [pltpu.make_async_copy(fields, fv, in_sem.at[0]),
             pltpu.make_async_copy(dep_row, drv, in_sem.at[1]),
             pltpu.make_async_copy(dep_col, dcv, in_sem.at[2]),
             pltpu.make_async_copy(weights, wv, in_sem.at[3])]
    for copy in loads:
        copy.start()
    barrier = pltpu.get_barrier_semaphore()
    for name in there:
        pl.semaphore_signal(barrier, inc=1, device_id=there[name], device_id_type=MESH)

    def tile(ref, lead, start, c):
        return ref[lead + (slice(start, start + SUB), slice(c * LANES, c * LANES + widths[c]))]

    loads[0].wait()
    for k in range(blocks):
        east = jnp.zeros((SUB, LANES), F32)
        west = jnp.zeros((SUB, LANES), F32)
        for f in range(nf):
            for l in range(nl):
                p = HALO * (f * nl + l)
                own = (lane >= p) & (lane < p + HALO)
                e = widen(tile(fv, (f, l), SUB * k, tiles - 1))
                east = jnp.where(own, roll(e, p - (tail - HALO), 1), east)
                west = jnp.where(own, roll(tile(fv, (f, l), SUB * k, 0), p, 1), west)
        strip[0, pl.ds(SUB * k, SUB), :] = east
        strip[1, pl.ds(SUB * k, SUB), :] = west

    def slab_of(side, g, l, c):
        a = tile(fv, (2 * g, l), 0 if side == 0 else last, c)
        b = tile(fv, (2 * g + 1, l), 0 if side == 0 else last, c)
        mask = sub_iota(a.shape) < HALO
        return jnp.where(mask, a, roll(b, HALO, 0)) if side == 0 else jnp.where(mask, roll(a, HALO, 0), b)

    for side in range(2):
        for l in range(nl):
            for c in range(tiles - 1):
                for g in range(2):
                    slab[side, l, 2 * c + g] = slab_of(side, g, l, c)
            pair = [slab_of(side, g, l, tiles - 1) for g in range(2)]
            slab[side, l, 2 * tiles - 2] = jnp.concatenate(pair, axis=-1)
    for edge in range(2):
        corner[0, edge] = strip[edge, 0:SUB, :]
        corner[1, edge] = roll(strip[edge, pl.ds(last, SUB), :], HALO, 0)

    for side, here in ((0, top), (1, bottom)):
        @pl.when(here)
        def _():
            for l in range(nl):
                for m in range(2 * tiles - 1):
                    slab[side, l, m] = flip4(slab[side, l, m])
            for edge in range(2):
                corner[side, edge] = flip4(corner[side, edge])

    for copy in loads[1:]:
        copy.wait()

    def zero_pads():
        for c in range(tiles):
            for f in range(nf):
                for t in range(SPAN):
                    sh[c, f, t, 0:SUB, :] = jnp.zeros((SUB, LANES), F32)
                    sh[c, f, t, pl.ds(SUB + rows, SUB), :] = jnp.zeros((SUB, LANES), F32)
        for m in range(2 * tiles - 1):
            for side in range(2):
                for t in range(SPAN):
                    tn[side, m, t, 0:SUB, :] = jnp.zeros((SUB, LANES), F32)
                    tn[side, m, t, 2 * SUB:3 * SUB, :] = jnp.zeros((SUB, LANES), F32)
        pw[...] = jnp.zeros(pw.shape, F32)

    def shifted(mid, left, right, t):
        d = t - HALO
        if d == 0:
            return mid
        if d < 0:
            return roll(mid if left is None else jnp.where(lane >= LANES + d, left, mid), -d, 1) if left is not None else jnp.where(
                lane < -d, 0.0, roll(mid, -d, 1))
        if right is None:
            return jnp.where(lane >= LANES - d, 0.0, roll(mid, -d, 1))
        return roll(jnp.where(lane < d, right, mid), -d, 1)

    def main():
        zero_pads()

        @pl.loop(0, nl)
        def _(l):
            for c in range(tiles):
                shape = (SUB, widths[c])
                ones = slice(0, widths[c])
                for k in range(blocks):
                    at = (l, slice(SUB * k, SUB * k + SUB), slice(c * LANES, c * LANES + widths[c]))
                    o_row = drv[at] - (band * rows + SUB * k - HALO + sub_iota(shape))
                    o_col = dcv[at] - (sector * cols + c * LANES - HALO + lane_iota(shape))
                    o_col = jnp.where(o_col > HALO, o_col - total_cols, o_col)
                    row_w = select_weights(o_row, [wv[(a,) + at] for a in range(4)])
                    col_w = select_weights(o_col, [wv[(4 + a,) + at] for a in range(4)])
                    for s in range(SPAN):
                        rc[l, c, s, pl.ds(SUB * k, SUB), ones] = row_w[s]
                        rc[l, c, SPAN + s, pl.ds(SUB * k, SUB), ones] = col_w[s]
                    if c == 0 or c == tiles - 1:
                        side = 0 if c == 0 else 1
                        own = (lane >= HALO * l) & (lane < HALO * l + HALO)
                        for i, x in enumerate(row_w + col_w):
                            x = widen(x)
                            if side:
                                x = roll(x, -(tail - HALO), 1)
                            x = pltpu.roll(x, HALO * l, 1)
                            spot = (side, i, pl.ds(SUB * k, SUB), slice(None))
                            pw[spot] = jnp.where(own, x, pw[spot])
                for f in range(nf):
                    for k in range(blocks):
                        mid = widen(tile(fv, (f, l), SUB * k, c))
                        left = tile(fv, (f, l), SUB * k, c - 1) if c else None
                        right = widen(tile(fv, (f, l), SUB * k, c + 1)) if c + 1 < tiles else None
                        for t in range(SPAN):
                            sh[c, f, t, pl.ds(SUB + SUB * k, SUB), :] = shifted(mid, left, right, t)
                col_t = [[rc[l, c, SPAN + t, pl.ds(k, SUB, stride=blocks), :] for t in range(SPAN)] for k in range(blocks)]
                for f in range(nf):
                    acc = [None] * blocks
                    for u in range(SPAN + blocks - 1):
                        x = [sh[c, f, t, pl.ds(HALO + u, SUB, stride=blocks), :] for t in range(SPAN)]
                        for k in range(blocks):
                            s = u - k
                            if 0 <= s < SPAN:
                                line = col_t[k][0] * x[0]
                                for t in range(1, SPAN):
                                    line = line + col_t[k][t] * x[t]
                                line = line * rc[l, c, s, pl.ds(k, SUB, stride=blocks), :]
                                acc[k] = line if acc[k] is None else acc[k] + line
                    for k in range(blocks):
                        ov[f, l, c, pl.ds(k, SUB, stride=blocks), :] = acc[k]

        for side in range(2):
            for i in range(2 * SPAN):
                for k in range(blocks):
                    spot = (side, i, pl.ds(SUB * k, SUB), slice(None))
                    x = pw[spot]
                    x = x + roll(x, HALO * nl, 1)
                    pw[spot] = x + roll(x, 2 * HALO * nl, 1)

    early = lax.rem(sector, EARLY_EVERY) == 0

    @pl.when(early)
    def _():
        main()

    pl.semaphore_wait(barrier, len(there))
    slot_n, slot_s = jnp.where(top, 0, 1), jnp.where(bottom, 1, 0)
    sends = []

    def send(src, dst, i, j, to):
        copy = pltpu.make_async_remote_copy(
            src_ref=src, dst_ref=dst, send_sem=send_sem.at[i], recv_sem=recv_sem.at[j],
            device_id=there[to], device_id_type=MESH)
        copy.start()
        sends.append(copy)

    send(strip.at[0], strip_in.at[0], 0, 0, "E")
    send(strip.at[1], strip_in.at[1], 1, 1, "W")
    for side, slot, names in ((0, slot_n, ("NE", "NW")), (1, slot_s, ("SE", "SW"))):
        for edge in range(2):
            n = 2 * side + edge
            send(corner.at[side, edge, pl.ds(0, HALO)], corner_in.at[slot, edge, pl.ds(0, HALO)], 2 + n, 2 + 2 * slot + edge, names[edge])
    send(slab.at[0], slab_in.at[slot_n], 6, 6 + slot_n, "N")
    send(slab.at[1], slab_in.at[slot_s], 7, 6 + slot_s, "S")

    @pl.when(jnp.logical_not(early))
    def _():
        main()

    def landed(ref, j):
        pltpu.make_async_copy(ref, ref, recv_sem.at[j]).wait()

    landed(slab_in.at[0], 6)
    landed(slab_in.at[1], 7)
    group = sub & (HALO - 1)

    def both(x, side):
        return jnp.where(sub < HALO, x, roll(x, HALO, 0)) if side == 0 else jnp.where(sub < HALO, roll(x, HALO, 0), x)

    @pl.loop(0, nl)
    def _(l):
        for side in range(2):
            base = 0 if side == 0 else last
            shifts = range(HALO) if side == 0 else range(HALO + 1, SPAN)
            ends = [slab_in[side, l, 2 * tiles - 2]] * 2
            ends[1] = roll(ends[1], -(LANES - tail), 1)
            for m in range(2 * tiles - 1):
                c, g = m // 2, m % 2
                mid = slab_in[side, l, m]
                for t in range(SPAN):
                    d = t - HALO
                    if c < tiles - 1:
                        left = slab_in[side, l, m - 2] if c else None
                        right = (slab_in[side, l, m + 2] if c + 2 < tiles else ends[g])
                        x = shifted(mid, left, right, t)
                    elif d <= 0:
                        x = roll(mid, -d, 1)
                        for h in range(2):
                            lo = h * (LANES - tail)
                            x = jnp.where((lane >= lo) & (lane < lo - d), roll(slab_in[side, l, m - 2 + h], lo - d, 1), x) if d else x
                    else:
                        inner = lane & (LANES // 2 - 1)
                        x = jnp.where(inner >= LANES // 2 - d, 0.0, roll(mid, -d, 1))
                    tn[side, m, t, SUB:2 * SUB, :] = x
            for c in range(tiles):
                def weight(i):
                    x = rc[l, c, i, pl.ds(base, SUB), 0:widths[c]]
                    if c == tiles - 1:
                        x = jnp.concatenate([x, x], axis=-1)
                    return both(x, side)

                col_w = [weight(SPAN + t) for t in range(SPAN)]
                row_w = {}
                for s in shifts:
                    valid = group + s < HALO if side == 0 else group + s >= SPAN
                    row_w[s] = jnp.where(valid, weight(s), 0.0)
                for g in range(2 if c < tiles - 1 else 1):
                    m = 2 * c + g
                    acc = None
                    for s in shifts:
                        first = SUB + s if side == 0 else s
                        line = None
                        for t in range(SPAN):
                            term = col_w[t] * tn[side, m, t, pl.ds(first, SUB), :]
                            line = term if line is None else line + term
                        line = line * row_w[s]
                        acc = line if acc is None else acc + line
                    keep = sub < HALO if side == 0 else sub >= HALO
                    for h in range(2 if c < tiles - 1 else 4):
                        part = acc
                        f = 2 * g + h if c < tiles - 1 else h
                        if c == tiles - 1 and h >= 2:
                            part = roll(part, -(LANES - tail), 1)
                        if side == 0:
                            part = part if f % 2 == 0 else roll(part, HALO, 0)
                        else:
                            part = part if f % 2 == 1 else roll(part, HALO, 0)
                        spot = (f, l, c, pl.ds(base, SUB), slice(None))
                        ov[spot] = ov[spot] + jnp.where(keep, part, 0.0)

    landed(strip_in.at[0], 0)
    landed(strip_in.at[1], 1)
    for side in range(2):
        for edge in range(2):
            landed(corner_in.at[side, edge, pl.ds(0, HALO)], 2 + 2 * side + edge)
    for edge in range(2):
        taps = range(HALO) if edge == 0 else range(HALO + 1, SPAN)
        for t in taps:
            d = t if edge == 0 else t - SPAN
            for k in range(blocks):
                xx[edge, t, pl.ds(SUB + SUB * k, SUB), :] = roll(strip_in[edge, pl.ds(SUB * k, SUB), :], -d, 1)
            xx[edge, t, HALO:SUB, :] = roll(corner_in[0, edge, 0:HALO, :], -d, 1)
            xx[edge, t, SUB + rows:SUB + rows + HALO, :] = roll(corner_in[1, edge, 0:HALO, :], -d, 1)
        col = lane & (HALO - 1)
        for k in range(blocks):
            col_w = {}
            for t in taps:
                valid = col + t < HALO if edge == 0 else col + t >= SPAN
                col_w[t] = jnp.where(valid, pw[edge, SPAN + t, pl.ds(k, SUB, stride=blocks), :], 0.0)
            acc = None
            for s in range(SPAN):
                line = None
                for t in taps:
                    term = col_w[t] * xx[edge, t, pl.ds(HALO + k + s, SUB, stride=blocks), :]
                    line = term if line is None else line + term
                line = line * pw[edge, s, pl.ds(k, SUB, stride=blocks), :]
                acc = line if acc is None else acc + line
            pd[edge, pl.ds(k, SUB, stride=blocks), :] = acc
    copies = []
    for f in range(nf):
        for l in range(nl):
            p = HALO * (f * nl + l)
            for k in range(blocks):
                at = pl.ds(SUB * k, SUB)
                for c in range(tiles):
                    x = ov[f, l, c, at, :]
                    if c == 0:
                        x = x + jnp.where(lane < HALO, roll(pd[0, at, :], -p, 1), 0.0)
                    if c == tiles - 1:
                        keep = (lane >= tail - HALO) & (lane < tail)
                        x = x + jnp.where(keep, roll(pd[1, at, :], tail - HALO - p, 1), 0.0)
                    fv[f, l, at, c * LANES:c * LANES + widths[c]] = x[:, :widths[c]]
        copy = pltpu.make_async_copy(fv.at[f], out.at[f], out_sem.at[f])
        copy.start()
        copies.append(copy)
    for copy in copies:
        copy.wait()
    for copy in sends:
        copy.wait_send()


def solution(mesh):
    nband, nsector = mesh.shape["lat"], mesh.shape["lon"]

    def body(fields, dep_row, dep_col, weights):
        nf, nl, rows, cols = fields.shape
        tiles = pl.cdiv(cols, LANES)
        dims = (nf, nl, rows, cols, nband, nsector, cols * nsector)
        vmem = lambda *shape: pltpu.VMEM(shape, F32)
        groups = 2 * tiles - 1
        return pl.pallas_call(
            functools.partial(kernel, dims),
            out_shape=jax.ShapeDtypeStruct(fields.shape, F32),
            in_specs=[pl.BlockSpec(memory_space=pltpu.HBM)] * 4,
            out_specs=pl.BlockSpec(memory_space=pltpu.HBM),
            scratch_shapes=[
                vmem(nf, nl, rows, cols),
                pltpu.VMEM((nl, rows, cols), jnp.int32),
                pltpu.VMEM((nl, rows, cols), jnp.int32),
                vmem(8, nl, rows, cols),
                vmem(nf, nl, tiles, rows, LANES),
                vmem(nl, tiles, 2 * SPAN, rows, LANES),
                vmem(tiles, nf, SPAN, rows + 2 * SUB, LANES),
                vmem(2, nl, groups, SUB, LANES), vmem(2, nl, groups, SUB, LANES),
                vmem(2, rows, LANES), vmem(2, rows, LANES),
                vmem(2, 2, SUB, LANES), vmem(2, 2, SUB, LANES),
                vmem(2, groups, SPAN, 3 * SUB, LANES),
                vmem(2, SPAN, rows + 2 * SUB, LANES),
                vmem(2, 2 * SPAN, rows, LANES),
                vmem(2, rows, LANES),
                pltpu.SemaphoreType.DMA((4,)), pltpu.SemaphoreType.DMA((nf,)),
                pltpu.SemaphoreType.DMA((8,)), pltpu.SemaphoreType.DMA((8,)),
            ],
            compiler_params=pltpu.CompilerParams(
                collective_id=0, has_side_effects=True, vmem_limit_bytes=67043328),
            name="advect",
        )(fields, dep_row, dep_col, weights)

    return jax.shard_map(
        body,
        mesh=mesh,
        in_specs=(
            P(None, None, "lat", "lon"),
            P(None, "lat", "lon"),
            P(None, "lat", "lon"),
            P(None, None, "lat", "lon"),
        ),
        out_specs=P(None, None, "lat", "lon"),
        check_vma=False,
    )
```

```python
import functools

import jax
import jax.numpy as jnp
from jax import lax
from jax.experimental import pallas as pl
from jax.experimental.pallas import tpu as pltpu
from jax.sharding import PartitionSpec as P

MESH = pl.DeviceIdType.MESH
F32 = jnp.float32
LANES = 128
SUB = 8
HALO = 4
SPAN = 2 * HALO
RUN = 4
PIECES = 3


def lane_iota(shape):
    return lax.broadcasted_iota(jnp.int32, shape, len(shape) - 1)


def sub_iota(shape):
    return lax.broadcasted_iota(jnp.int32, shape, len(shape) - 2)


def roll(x, shift, axis):
    size = x.shape[axis]
    return pltpu.roll(x, shift % size, axis) if shift % size else x


def widen(x):
    width = x.shape[-1]
    if width == LANES:
        return x
    return jnp.concatenate([x, jnp.zeros(x.shape[:-1] + (LANES - width,), x.dtype)], axis=-1)


def neighbours(band, sector, nband, nsector):
    east = lax.rem(sector + 1, nsector)
    west = lax.rem(sector + nsector - 1, nsector)
    top, bottom = band == 0, band == nband - 1
    north, south = jnp.where(top, band, band - 1), jnp.where(bottom, band, band + 1)
    half = nsector // 2
    turn_n, turn_s = jnp.where(top, half, 0), jnp.where(bottom, half, 0)

    def at(row, col, turn):
        return (row, lax.rem(col + turn, nsector))

    return {
        "E": (band, east), "W": (band, west),
        "N": at(north, sector, turn_n), "S": at(south, sector, turn_s),
        "NE": at(north, east, turn_n), "NW": at(north, west, turn_n),
        "SE": at(south, east, turn_s), "SW": at(south, west, turn_s),
    }


def select_weights(offset, taps):
    masks = [offset == o for o in range(HALO + 1)]
    out = []
    for s in range(SPAN):
        term = jnp.zeros(offset.shape, F32)
        for a in range(4):
            if 0 <= s - a <= HALO:
                term = jnp.where(masks[s - a], taps[a], term)
        out.append(term)
    return out


def flip4(x):
    i = sub_iota(x.shape)
    x = jnp.where((i & 1) == 1, roll(x, 1, 0), roll(x, -1, 0))
    return jnp.where((i & 2) == 2, roll(x, 2, 0), roll(x, -2, 0))


def kernel(dims, fields, dep_row, dep_col, weights, out,
           fv, drv, dcv, wv, ov, rc, sh, slab, slab_in, strip, strip_in, corner, corner_in,
           tn, nw, xx, pw, pd, in_sem, send_sem, recv_sem):
    nf, nl, rows, cols, nband, nsector, total_cols = dims
    band, sector = lax.axis_index("lat"), lax.axis_index("lon")
    there = neighbours(band, sector, nband, nsector)
    top, bottom = band == 0, band == nband - 1
    tiles = pl.cdiv(cols, LANES)
    tail = cols - (tiles - 1) * LANES
    widths = [LANES] * (tiles - 1) + [tail]
    blocks = rows // SUB
    last = rows - SUB
    lane = lane_iota((SUB, LANES))
    sub = sub_iota((SUB, LANES))

    loads = [pltpu.make_async_copy(fields, fv, in_sem.at[0]),
             pltpu.make_async_copy(dep_row, drv, in_sem.at[1]),
             pltpu.make_async_copy(dep_col, dcv, in_sem.at[2]),
             pltpu.make_async_copy(weights, wv, in_sem.at[3])]
    for copy in loads:
        copy.start()
    barrier = pltpu.get_barrier_semaphore()
    for name in there:
        pl.semaphore_signal(barrier, inc=1, device_id=there[name], device_id_type=MESH)

    groups = 2 * tiles - 1

    def row_shifts(side):
        return range(HALO + 1, SPAN) if side else range(HALO)

    def tile(ref, lead, start, c):
        return ref[lead + (slice(start, start + SUB), slice(c * LANES, c * LANES + widths[c]))]

    def zero_pads():
        for c in range(tiles):
            for f in range(nf):
                for t in range(SPAN):
                    sh[c, f, t, 0:SUB, :] = jnp.zeros((SUB, LANES), F32)
                    sh[c, f, t, pl.ds(SUB + rows, SUB), :] = jnp.zeros((SUB, LANES), F32)
        for n in range(nl // PIECES):
            for m in range(groups):
                for t in range(SPAN):
                    tn[n, 0, m, t, 2 * SUB:3 * SUB, :] = jnp.zeros((SUB, LANES), F32)
                    tn[n, 1, m, t, 0:SUB, :] = jnp.zeros((SUB, LANES), F32)
        pw[...] = jnp.zeros(pw.shape, F32)

    zero_pads()

    loads[0].wait()
    for k in range(blocks):
        east = jnp.zeros((SUB, LANES), F32)
        west = jnp.zeros((SUB, LANES), F32)
        for f in range(nf):
            for l in range(nl):
                p = HALO * (f * nl + l)
                own = (lane >= p) & (lane < p + HALO)
                e = widen(tile(fv, (f, l), SUB * k, tiles - 1))
                east = jnp.where(own, roll(e, p - (tail - HALO), 1), east)
                west = jnp.where(own, roll(tile(fv, (f, l), SUB * k, 0), p, 1), west)
        strip[0, pl.ds(SUB * k, SUB), :] = east
        strip[1, pl.ds(SUB * k, SUB), :] = west

    def slab_of(side, g, l, c):
        a = tile(fv, (2 * g, l), 0 if side == 0 else last, c)
        b = tile(fv, (2 * g + 1, l), 0 if side == 0 else last, c)
        mask = sub_iota(a.shape) < HALO
        return jnp.where(mask, a, roll(b, HALO, 0)) if side == 0 else jnp.where(mask, roll(a, HALO, 0), b)

    for side in range(2):
        for l in range(nl):
            for c in range(tiles - 1):
                for g in range(2):
                    slab[side, l, 2 * c + g] = slab_of(side, g, l, c)
            pair = [slab_of(side, g, l, tiles - 1) for g in range(2)]
            slab[side, l, 2 * tiles - 2] = jnp.concatenate(pair, axis=-1)
    for edge in range(2):
        corner[0, edge] = strip[edge, 0:SUB, :]
        corner[1, edge] = roll(strip[edge, pl.ds(last, SUB), :], HALO, 0)

    for side, here in ((0, top), (1, bottom)):
        @pl.when(here)
        def _():
            for l in range(nl):
                for m in range(2 * tiles - 1):
                    slab[side, l, m] = flip4(slab[side, l, m])
            for edge in range(2):
                corner[side, edge] = flip4(corner[side, edge])

    for copy in loads[1:]:
        copy.wait()

    def shifted(mid, left, right, t):
        d = t - HALO
        if d == 0:
            return mid
        if d < 0:
            return roll(mid if left is None else jnp.where(lane >= LANES + d, left, mid), -d, 1) if left is not None else jnp.where(
                lane < -d, 0.0, roll(mid, -d, 1))
        if right is None:
            return jnp.where(lane >= LANES - d, 0.0, roll(mid, -d, 1))
        return roll(jnp.where(lane < d, right, mid), -d, 1)

    def levels(begin, end):
        @pl.loop(begin, end)
        def _(l):
            for c in range(tiles):
                shape = (SUB, widths[c])
                ones = slice(0, widths[c])
                for k in range(blocks):
                    at = (l, slice(SUB * k, SUB * k + SUB), slice(c * LANES, c * LANES + widths[c]))
                    o_row = drv[at] - (band * rows + SUB * k - HALO + sub_iota(shape))
                    o_col = dcv[at] - (sector * cols + c * LANES - HALO + lane_iota(shape))
                    o_col = jnp.where(o_col > HALO, o_col - total_cols, o_col)
                    row_w = select_weights(o_row, [wv[(a,) + at] for a in range(4)])
                    col_w = select_weights(o_col, [wv[(4 + a,) + at] for a in range(4)])
                    for s in range(SPAN):
                        rc[l, c, s, pl.ds(SUB * k, SUB), ones] = row_w[s]
                        rc[l, c, SPAN + s, pl.ds(SUB * k, SUB), ones] = col_w[s]
                    if c == 0 or c == tiles - 1:
                        side = 0 if c == 0 else 1
                        own = (lane >= HALO * l) & (lane < HALO * l + HALO)
                        for i, x in enumerate(row_w + col_w):
                            x = widen(x)
                            if side:
                                x = roll(x, -(tail - HALO), 1)
                            x = pltpu.roll(x, HALO * l, 1)
                            spot = (side, i, pl.ds(SUB * k, SUB), slice(None))
                            pw[spot] = jnp.where(own, x, pw[spot])
                for f in range(nf):
                    for k in range(blocks):
                        mid = widen(tile(fv, (f, l), SUB * k, c))
                        left = tile(fv, (f, l), SUB * k, c - 1) if c else None
                        right = widen(tile(fv, (f, l), SUB * k, c + 1)) if c + 1 < tiles else None
                        for t in range(SPAN):
                            sh[c, f, t, pl.ds(SUB + SUB * k, SUB), :] = shifted(mid, left, right, t)
                col_t = [[rc[l, c, SPAN + t, pl.ds(k, SUB, stride=blocks), :] for t in range(SPAN)] for k in range(blocks)]
                for f in range(nf):
                    acc = [None] * blocks
                    for u in range(SPAN + blocks - 1):
                        x = [sh[c, f, t, pl.ds(HALO + u, SUB, stride=blocks), :] for t in range(SPAN)]
                        for k in range(blocks):
                            s = u - k
                            if 0 <= s < SPAN:
                                line = col_t[k][0] * x[0]
                                for t in range(1, SPAN):
                                    line = line + col_t[k][t] * x[t]
                                line = line * rc[l, c, s, pl.ds(k, SUB, stride=blocks), :]
                                acc[k] = line if acc[k] is None else acc[k] + line
                    for k in range(blocks):
                        ov[f, l, c, pl.ds(k, SUB, stride=blocks), :] = acc[k]

            for side in range(2):
                for c in range(tiles):
                    shifts = row_shifts(side)
                    for n, i in enumerate([SPAN + t for t in range(SPAN)] + list(shifts)):
                        x = rc[l, c, i, pl.ds(side * last, SUB), 0:widths[c]]
                        x = jnp.concatenate([x, x], axis=-1) if c == tiles - 1 else x
                        turned = roll(x, HALO, 0)
                        x = jnp.where(sub < HALO, turned, x) if side else jnp.where(sub < HALO, x, turned)
                        if i < SPAN:
                            row = (sub & (HALO - 1)) + i
                            x = jnp.where(row >= SPAN if side else row < HALO, x, 0.0)
                        nw[l, side, c, n] = x

    def spread():
        for side in range(2):
            for i in range(2 * SPAN):
                for k in range(blocks):
                    spot = (side, i, pl.ds(SUB * k, SUB), slice(None))
                    x = pw[spot]
                    x = x + roll(x, HALO * nl, 1)
                    pw[spot] = x + roll(x, 2 * HALO * nl, 1)

    place = lax.rem(sector, RUN)
    ahead = jnp.where(place == 0, nl, jnp.where(place == 1, nl // 3, jnp.where(place == 2, nl // 6, 0)))
    ahead = jnp.where(band + sector == 0, 0, ahead)
    levels(0, ahead)
    pl.semaphore_wait(barrier, len(there))
    slot_n, slot_s = jnp.where(top, 0, 1), jnp.where(bottom, 1, 0)

    def send(src, dst, i, j, to):
        return pltpu.make_async_remote_copy(
            src_ref=src, dst_ref=dst, send_sem=send_sem.at[i], recv_sem=recv_sem.at[j],
            device_id=there[to], device_id_type=MESH)

    per = nl // PIECES
    sends = []
    for edge in range(2):
        sends.append(send(strip.at[edge], strip_in.at[edge], edge, edge, "EW"[edge]))
    for side, slot, row in ((0, slot_n, "N"), (1, slot_s, "S")):
        for edge in range(2):
            sends.append(send(corner.at[side, edge, pl.ds(0, HALO)], corner_in.at[slot, edge, pl.ds(0, HALO)],
                              2 + 2 * side + edge, 2 + 2 * slot + edge, row + "EW"[edge]))
    for q in range(PIECES):
        piece = pl.ds(per * q, per)
        for side, slot, to in ((0, slot_n, "N"), (1, slot_s, "S")):
            sends.append(send(slab.at[side, piece], slab_in.at[slot, piece],
                              6 + PIECES * side + q, 6 + PIECES * slot + q, to))
    for copy in sends:
        copy.start()

    levels(ahead, nl)
    spread()

    def landed(ref, j):
        pltpu.make_async_copy(ref, ref, recv_sem.at[j]).wait()

    def columns(edge):
        landed(strip_in.at[edge], edge)
        for side in range(2):
            landed(corner_in.at[side, edge, pl.ds(0, HALO)], 2 + 2 * side + edge)
        taps = range(HALO) if edge == 0 else range(HALO + 1, SPAN)
        for t in taps:
            d = t if edge == 0 else t - SPAN
            for k in range(blocks):
                xx[edge, t, pl.ds(SUB + SUB * k, SUB), :] = roll(strip_in[edge, pl.ds(SUB * k, SUB), :], -d, 1)
            xx[edge, t, HALO:SUB, :] = roll(corner_in[0, edge, 0:HALO, :], -d, 1)
            xx[edge, t, SUB + rows:SUB + rows + HALO, :] = roll(corner_in[1, edge, 0:HALO, :], -d, 1)
        col = lane & (HALO - 1)
        for k in range(blocks):
            col_w = {}
            for t in taps:
                valid = col + t < HALO if edge == 0 else col + t >= SPAN
                col_w[t] = jnp.where(valid, pw[edge, SPAN + t, pl.ds(k, SUB, stride=blocks), :], 0.0)
            acc = None
            for s in range(SPAN):
                line = None
                for t in taps:
                    term = col_w[t] * xx[edge, t, pl.ds(HALO + k + s, SUB, stride=blocks), :]
                    line = term if line is None else line + term
                line = line * pw[edge, s, pl.ds(k, SUB, stride=blocks), :]
                acc = line if acc is None else acc + line
            pd[edge, pl.ds(k, SUB, stride=blocks), :] = acc
        for k in range(blocks):
            at = pl.ds(SUB * k, SUB)
            extra = pd[edge, at, :]
            for f in range(nf):
                for l in range(nl):
                    p = HALO * (f * nl + l)
                    if edge == 0:
                        x = ov[f, l, 0, at, :]
                        out[f, l, at, 0:LANES] = x + jnp.where(lane < HALO, roll(extra, -p, 1), 0.0)
                        continue
                    for c in range(1, tiles):
                        x = ov[f, l, c, at, :]
                        if c == tiles - 1:
                            keep = (lane >= tail - HALO) & (lane < tail)
                            x = x + jnp.where(keep, roll(extra, tail - HALO - p, 1), 0.0)
                        out[f, l, at, c * LANES:c * LANES + widths[c]] = x[:, :widths[c]]

    columns(1)
    for l in range(nl):
        if l % per == 0:
            for side in range(2):
                landed(slab_in.at[side, pl.ds(l, per)], 6 + PIECES * side + l // per)
        for side in range(2):
            buf = tn.at[l % per, side]
            base = side * last
            ends = [slab_in[side, l, groups - 1]] * 2
            ends[1] = roll(ends[1], -tail, 1)
            for m in range(groups):
                c, g = m // 2, m % 2
                mid = slab_in[side, l, m]
                for t in range(SPAN):
                    d = t - HALO
                    if c < tiles - 1:
                        left = slab_in[side, l, m - 2] if c else None
                        right = slab_in[side, l, m + 2] if c + 2 < tiles else ends[g]
                        x = shifted(mid, left, right, t)
                    elif d <= 0:
                        x = roll(mid, -d, 1)
                        for h in range(2):
                            lo = h * tail
                            edge = roll(slab_in[side, l, m - 2 + h], lo - d, 1)
                            x = jnp.where((lane >= lo) & (lane < lo - d), edge, x) if d else x
                    else:
                        x = jnp.where((lane & (tail - 1)) >= tail - d, 0.0, roll(mid, -d, 1))
                    buf[m, t, SUB:2 * SUB, :] = x
            for c in range(tiles):
                shifts = row_shifts(side)
                col_w = [nw[l, side, c, t] for t in range(SPAN)]
                row_w = [nw[l, side, c, SPAN + n] for n in range(len(shifts))]
                for g in range(2 if c < tiles - 1 else 1):
                    m = 2 * c + g
                    acc = None
                    for n, s in enumerate(shifts):
                        start = SUB + s if side == 0 else s
                        line = None
                        for t in range(SPAN):
                            term = col_w[t] * buf[m, t, pl.ds(start, SUB), :]
                            line = term if line is None else line + term
                        line = line * row_w[n]
                        acc = line if acc is None else acc + line
                    keep = sub < HALO if side == 0 else sub >= HALO
                    for h in range(2 if c < tiles - 1 else 4):
                        f = 2 * g + h if c < tiles - 1 else h
                        part = roll(acc, -tail, 1) if h >= 2 else acc
                        part = part if f % 2 == side else roll(part, HALO, 0)
                        part = jnp.where(keep, part, 0.0)
                        if c == 0:
                            spot = (f, l, c, pl.ds(base, SUB), slice(None))
                            ov[spot] = ov[spot] + part
                        else:
                            spot = (f, l, pl.ds(base, SUB), slice(c * LANES, c * LANES + widths[c]))
                            out[spot] = out[spot] + part[:, :widths[c]]
    columns(0)
    for copy in sends:
        copy.wait_send()


def solution(mesh):
    nband, nsector = mesh.shape["lat"], mesh.shape["lon"]

    def body(fields, dep_row, dep_col, weights):
        nf, nl, rows, cols = fields.shape
        tiles = pl.cdiv(cols, LANES)
        dims = (nf, nl, rows, cols, nband, nsector, cols * nsector)
        vmem = lambda *shape: pltpu.VMEM(shape, F32)
        groups = 2 * tiles - 1
        return pl.pallas_call(
            functools.partial(kernel, dims),
            out_shape=jax.ShapeDtypeStruct(fields.shape, F32),
            in_specs=[pl.BlockSpec(memory_space=pltpu.HBM)] * 4,
            out_specs=pl.BlockSpec(memory_space=pltpu.VMEM),
            scratch_shapes=[
                vmem(nf, nl, rows, cols),
                pltpu.VMEM((nl, rows, cols), jnp.int32),
                pltpu.VMEM((nl, rows, cols), jnp.int32),
                vmem(8, nl, rows, cols),
                vmem(nf, nl, tiles, rows, LANES),
                vmem(nl, tiles, 2 * SPAN, rows, LANES),
                vmem(tiles, nf, SPAN, rows + 2 * SUB, LANES),
                vmem(2, nl, groups, SUB, LANES), vmem(2, nl, groups, SUB, LANES),
                vmem(2, rows, LANES), vmem(2, rows, LANES),
                vmem(2, 2, SUB, LANES), vmem(2, 2, SUB, LANES),
                vmem(nl // PIECES, 2, groups, SPAN, 3 * SUB, LANES),
                vmem(nl, 2, tiles, SPAN + HALO, SUB, LANES),
                vmem(2, SPAN, rows + 2 * SUB, LANES),
                vmem(2, 2 * SPAN, rows, LANES),
                vmem(2, rows, LANES),
                pltpu.SemaphoreType.DMA((4,)),
                pltpu.SemaphoreType.DMA((6 + 2 * PIECES,)), pltpu.SemaphoreType.DMA((6 + 2 * PIECES,)),
            ],
            compiler_params=pltpu.CompilerParams(
                collective_id=0, has_side_effects=True, vmem_limit_bytes=40 << 20),
            name="advect",
        )(*[pltpu.with_memory_space_constraint(x, pltpu.HBM) for x in (fields, dep_row, dep_col, weights)])

    return jax.shard_map(
        body,
        mesh=mesh,
        in_specs=(
            P(None, None, "lat", "lon"),
            P(None, "lat", "lon"),
            P(None, "lat", "lon"),
            P(None, None, "lat", "lon"),
        ),
        out_specs=P(None, None, "lat", "lon"),
        check_vma=False,
    )
```

```python
import functools

import jax
import jax.numpy as jnp
from jax import lax
from jax.experimental import pallas as pl
from jax.experimental.pallas import tpu as pltpu
from jax.sharding import PartitionSpec as P

MESH = pl.DeviceIdType.MESH
F32 = jnp.float32
LANES = 128
SUB = 8
HALO = 4
SPAN = 2 * HALO
RUN = 4
PIECES = 6


def lane_iota(shape):
    return lax.broadcasted_iota(jnp.int32, shape, len(shape) - 1)


def sub_iota(shape):
    return lax.broadcasted_iota(jnp.int32, shape, len(shape) - 2)


def roll(x, shift, axis):
    size = x.shape[axis]
    return pltpu.roll(x, shift % size, axis) if shift % size else x


def widen(x):
    width = x.shape[-1]
    if width == LANES:
        return x
    return jnp.concatenate([x, jnp.zeros(x.shape[:-1] + (LANES - width,), x.dtype)], axis=-1)


def neighbours(band, sector, nband, nsector):
    east = lax.rem(sector + 1, nsector)
    west = lax.rem(sector + nsector - 1, nsector)
    top, bottom = band == 0, band == nband - 1
    north, south = jnp.where(top, band, band - 1), jnp.where(bottom, band, band + 1)
    half = nsector // 2
    turn_n, turn_s = jnp.where(top, half, 0), jnp.where(bottom, half, 0)

    def at(row, col, turn):
        return (row, lax.rem(col + turn, nsector))

    return {
        "E": (band, east), "W": (band, west),
        "N": at(north, sector, turn_n), "S": at(south, sector, turn_s),
        "NE": at(north, east, turn_n), "NW": at(north, west, turn_n),
        "SE": at(south, east, turn_s), "SW": at(south, west, turn_s),
    }


def select_weights(offset, taps):
    masks = [offset == o for o in range(HALO + 1)]
    out = []
    for s in range(SPAN):
        term = jnp.zeros(offset.shape, F32)
        for a in range(4):
            if 0 <= s - a <= HALO:
                term = jnp.where(masks[s - a], taps[a], term)
        out.append(term)
    return out


def flip4(x):
    i = sub_iota(x.shape)
    x = jnp.where((i & 1) == 1, roll(x, 1, 0), roll(x, -1, 0))
    return jnp.where((i & 2) == 2, roll(x, 2, 0), roll(x, -2, 0))


def kernel(dims, fields, dep_row, dep_col, weights, out,
           fv, drv, dcv, wv, ov, rc, sh, slab, slab_in, strip, strip_in, corner, corner_in,
           tn, nw, xx, pw, pd, in_sem, send_sem, recv_sem):
    nf, nl, rows, cols, nband, nsector, total_cols = dims
    band, sector = lax.axis_index("lat"), lax.axis_index("lon")
    there = neighbours(band, sector, nband, nsector)
    top, bottom = band == 0, band == nband - 1
    tiles = pl.cdiv(cols, LANES)
    tail = cols - (tiles - 1) * LANES
    widths = [LANES] * (tiles - 1) + [tail]
    blocks = rows // SUB
    last = rows - SUB
    lane = lane_iota((SUB, LANES))
    sub = sub_iota((SUB, LANES))

    loads = [pltpu.make_async_copy(fields, fv, in_sem.at[0]),
             pltpu.make_async_copy(dep_row, drv, in_sem.at[1]),
             pltpu.make_async_copy(dep_col, dcv, in_sem.at[2]),
             pltpu.make_async_copy(weights, wv, in_sem.at[3])]
    for copy in loads:
        copy.start()
    barrier = pltpu.get_barrier_semaphore()
    for name in there:
        pl.semaphore_signal(barrier, inc=1, device_id=there[name], device_id_type=MESH)

    groups = 2 * tiles - 1

    def row_shifts(side):
        return range(HALO + 1, SPAN) if side else range(HALO)

    def tile(ref, lead, start, c):
        return ref[lead + (slice(start, start + SUB), slice(c * LANES, c * LANES + widths[c]))]

    def zero_pads():
        for c in range(tiles):
            for f in range(nf):
                for t in range(SPAN):
                    sh[c, f, t, 0:SUB, :] = jnp.zeros((SUB, LANES), F32)
                    sh[c, f, t, pl.ds(SUB + rows, SUB), :] = jnp.zeros((SUB, LANES), F32)
        for n in range(nl // PIECES):
            for m in range(groups):
                for t in range(SPAN):
                    tn[n, 0, m, t, 2 * SUB:3 * SUB, :] = jnp.zeros((SUB, LANES), F32)
                    tn[n, 1, m, t, 0:SUB, :] = jnp.zeros((SUB, LANES), F32)
        pw[...] = jnp.zeros(pw.shape, F32)

    zero_pads()

    loads[0].wait()
    for k in range(blocks):
        east = jnp.zeros((SUB, LANES), F32)
        west = jnp.zeros((SUB, LANES), F32)
        for f in range(nf):
            for l in range(nl):
                p = HALO * (f * nl + l)
                own = (lane >= p) & (lane < p + HALO)
                e = widen(tile(fv, (f, l), SUB * k, tiles - 1))
                east = jnp.where(own, roll(e, p - (tail - HALO), 1), east)
                west = jnp.where(own, roll(tile(fv, (f, l), SUB * k, 0), p, 1), west)
        strip[0, pl.ds(SUB * k, SUB), :] = east
        strip[1, pl.ds(SUB * k, SUB), :] = west

    def slab_of(side, g, l, c):
        a = tile(fv, (2 * g, l), 0 if side == 0 else last, c)
        b = tile(fv, (2 * g + 1, l), 0 if side == 0 else last, c)
        mask = sub_iota(a.shape) < HALO
        return jnp.where(mask, a, roll(b, HALO, 0)) if side == 0 else jnp.where(mask, roll(a, HALO, 0), b)

    for side in range(2):
        for l in range(nl):
            for c in range(tiles - 1):
                for g in range(2):
                    slab[side, l, 2 * c + g] = slab_of(side, g, l, c)
            pair = [slab_of(side, g, l, tiles - 1) for g in range(2)]
            slab[side, l, 2 * tiles - 2] = jnp.concatenate(pair, axis=-1)
    for edge in range(2):
        corner[0, edge] = strip[edge, 0:SUB, :]
        corner[1, edge] = roll(strip[edge, pl.ds(last, SUB), :], HALO, 0)

    for side, here in ((0, top), (1, bottom)):
        @pl.when(here)
        def _():
            for l in range(nl):
                for m in range(2 * tiles - 1):
                    slab[side, l, m] = flip4(slab[side, l, m])
            for edge in range(2):
                corner[side, edge] = flip4(corner[side, edge])

    for copy in loads[1:]:
        copy.wait()

    def shifted(mid, left, right, t):
        d = t - HALO
        if d == 0:
            return mid
        if d < 0:
            return roll(mid if left is None else jnp.where(lane >= LANES + d, left, mid), -d, 1) if left is not None else jnp.where(
                lane < -d, 0.0, roll(mid, -d, 1))
        if right is None:
            return jnp.where(lane >= LANES - d, 0.0, roll(mid, -d, 1))
        return roll(jnp.where(lane < d, right, mid), -d, 1)

    def levels(begin, end):
        @pl.loop(begin, end)
        def _(l):
            for c in range(tiles):
                shape = (SUB, widths[c])
                ones = slice(0, widths[c])
                for k in range(blocks):
                    at = (l, slice(SUB * k, SUB * k + SUB), slice(c * LANES, c * LANES + widths[c]))
                    o_row = drv[at] - (band * rows + SUB * k - HALO + sub_iota(shape))
                    o_col = dcv[at] - (sector * cols + c * LANES - HALO + lane_iota(shape))
                    o_col = jnp.where(o_col > HALO, o_col - total_cols, o_col)
                    row_w = select_weights(o_row, [wv[(a,) + at] for a in range(4)])
                    col_w = select_weights(o_col, [wv[(4 + a,) + at] for a in range(4)])
                    for s in range(SPAN):
                        rc[l, c, s, pl.ds(SUB * k, SUB), ones] = row_w[s]
                        rc[l, c, SPAN + s, pl.ds(SUB * k, SUB), ones] = col_w[s]
                    if c == 0 or c == tiles - 1:
                        side = 0 if c == 0 else 1
                        own = (lane >= HALO * l) & (lane < HALO * l + HALO)
                        for i, x in enumerate(row_w + col_w):
                            x = widen(x)
                            if side:
                                x = roll(x, -(tail - HALO), 1)
                            x = pltpu.roll(x, HALO * l, 1)
                            spot = (side, i, pl.ds(SUB * k, SUB), slice(None))
                            pw[spot] = jnp.where(own, x, pw[spot])
                for f in range(nf):
                    for k in range(blocks):
                        mid = widen(tile(fv, (f, l), SUB * k, c))
                        left = tile(fv, (f, l), SUB * k, c - 1) if c else None
                        right = widen(tile(fv, (f, l), SUB * k, c + 1)) if c + 1 < tiles else None
                        for t in range(SPAN):
                            sh[c, f, t, pl.ds(SUB + SUB * k, SUB), :] = shifted(mid, left, right, t)
                col_t = [[rc[l, c, SPAN + t, pl.ds(k, SUB, stride=blocks), :] for t in range(SPAN)] for k in range(blocks)]
                for f in range(nf):
                    acc = [None] * blocks
                    for u in range(SPAN + blocks - 1):
                        x = [sh[c, f, t, pl.ds(HALO + u, SUB, stride=blocks), :] for t in range(SPAN)]
                        for k in range(blocks):
                            s = u - k
                            if 0 <= s < SPAN:
                                line = col_t[k][0] * x[0]
                                for t in range(1, SPAN):
                                    line = line + col_t[k][t] * x[t]
                                line = line * rc[l, c, s, pl.ds(k, SUB, stride=blocks), :]
                                acc[k] = line if acc[k] is None else acc[k] + line
                    for k in range(blocks):
                        ov[f, l, c, pl.ds(k, SUB, stride=blocks), :] = acc[k]

            for side in range(2):
                for c in range(tiles):
                    shifts = row_shifts(side)
                    for n, i in enumerate([SPAN + t for t in range(SPAN)] + list(shifts)):
                        x = rc[l, c, i, pl.ds(side * last, SUB), 0:widths[c]]
                        x = jnp.concatenate([x, x], axis=-1) if c == tiles - 1 else x
                        turned = roll(x, HALO, 0)
                        x = jnp.where(sub < HALO, turned, x) if side else jnp.where(sub < HALO, x, turned)
                        if i < SPAN:
                            row = (sub & (HALO - 1)) + i
                            x = jnp.where(row >= SPAN if side else row < HALO, x, 0.0)
                        nw[l, side, c, n] = x

    def spread():
        for side in range(2):
            for i in range(2 * SPAN):
                for k in range(blocks):
                    spot = (side, i, pl.ds(SUB * k, SUB), slice(None))
                    x = pw[spot]
                    x = x + roll(x, HALO * nl, 1)
                    pw[spot] = x + roll(x, 2 * HALO * nl, 1)

    place = lax.rem(sector, RUN)
    ahead = jnp.where(place == 0, nl, jnp.where(place == 1, nl // 3, jnp.where(place == 2, nl // 6, 0)))
    ahead = jnp.where(band + sector == 0, 0, ahead)
    levels(0, ahead)
    pl.semaphore_wait(barrier, len(there))
    slot_n, slot_s = jnp.where(top, 0, 1), jnp.where(bottom, 1, 0)

    def send(src, dst, i, j, to):
        return pltpu.make_async_remote_copy(
            src_ref=src, dst_ref=dst, send_sem=send_sem.at[i], recv_sem=recv_sem.at[j],
            device_id=there[to], device_id_type=MESH)

    per = nl // PIECES
    sends = []
    for edge in range(2):
        sends.append(send(strip.at[edge], strip_in.at[edge], edge, edge, "EW"[edge]))
    for side, slot, row in ((0, slot_n, "N"), (1, slot_s, "S")):
        for edge in range(2):
            sends.append(send(corner.at[side, edge, pl.ds(0, HALO)], corner_in.at[slot, edge, pl.ds(0, HALO)],
                              2 + 2 * side + edge, 2 + 2 * slot + edge, row + "EW"[edge]))
    for q in range(PIECES):
        piece = pl.ds(per * q, per)
        for side, slot, to in ((0, slot_n, "N"), (1, slot_s, "S")):
            sends.append(send(slab.at[side, piece], slab_in.at[slot, piece],
                              6 + PIECES * side + q, 6 + PIECES * slot + q, to))
    for copy in sends:
        copy.start()

    levels(ahead, nl)
    spread()

    def landed(ref, j):
        pltpu.make_async_copy(ref, ref, recv_sem.at[j]).wait()

    def columns(edge):
        landed(strip_in.at[edge], edge)
        for side in range(2):
            landed(corner_in.at[side, edge, pl.ds(0, HALO)], 2 + 2 * side + edge)
        taps = range(HALO) if edge == 0 else range(HALO + 1, SPAN)
        for t in taps:
            d = t if edge == 0 else t - SPAN
            for k in range(blocks):
                xx[edge, t, pl.ds(SUB + SUB * k, SUB), :] = roll(strip_in[edge, pl.ds(SUB * k, SUB), :], -d, 1)
            xx[edge, t, HALO:SUB, :] = roll(corner_in[0, edge, 0:HALO, :], -d, 1)
            xx[edge, t, SUB + rows:SUB + rows + HALO, :] = roll(corner_in[1, edge, 0:HALO, :], -d, 1)
        col = lane & (HALO - 1)
        for k in range(blocks):
            col_w = {}
            for t in taps:
                valid = col + t < HALO if edge == 0 else col + t >= SPAN
                col_w[t] = jnp.where(valid, pw[edge, SPAN + t, pl.ds(k, SUB, stride=blocks), :], 0.0)
            acc = None
            for s in range(SPAN):
                line = None
                for t in taps:
                    term = col_w[t] * xx[edge, t, pl.ds(HALO + k + s, SUB, stride=blocks), :]
                    line = term if line is None else line + term
                line = line * pw[edge, s, pl.ds(k, SUB, stride=blocks), :]
                acc = line if acc is None else acc + line
            pd[edge, pl.ds(k, SUB, stride=blocks), :] = acc
        for k in range(blocks):
            at = pl.ds(SUB * k, SUB)
            extra = pd[edge, at, :]
            for f in range(nf):
                for l in range(nl):
                    p = HALO * (f * nl + l)
                    if edge == 0:
                        x = ov[f, l, 0, at, :]
                        out[f, l, at, 0:LANES] = x + jnp.where(lane < HALO, roll(extra, -p, 1), 0.0)
                        continue
                    for c in range(1, tiles):
                        x = ov[f, l, c, at, :]
                        if c == tiles - 1:
                            keep = (lane >= tail - HALO) & (lane < tail)
                            x = x + jnp.where(keep, roll(extra, tail - HALO - p, 1), 0.0)
                        out[f, l, at, c * LANES:c * LANES + widths[c]] = x[:, :widths[c]]

    columns(1)
    for l in range(nl):
        if l % per == 0:
            for side in range(2):
                landed(slab_in.at[side, pl.ds(l, per)], 6 + PIECES * side + l // per)
        for side in range(2):
            buf = tn.at[l % per, side]
            base = side * last
            ends = [slab_in[side, l, groups - 1]] * 2
            ends[1] = roll(ends[1], -tail, 1)
            for m in range(groups):
                c, g = m // 2, m % 2
                mid = slab_in[side, l, m]
                for t in range(SPAN):
                    d = t - HALO
                    if c < tiles - 1:
                        left = slab_in[side, l, m - 2] if c else None
                        right = slab_in[side, l, m + 2] if c + 2 < tiles else ends[g]
                        x = shifted(mid, left, right, t)
                    elif d <= 0:
                        x = roll(mid, -d, 1)
                        for h in range(2):
                            lo = h * tail
                            edge = roll(slab_in[side, l, m - 2 + h], lo - d, 1)
                            x = jnp.where((lane >= lo) & (lane < lo - d), edge, x) if d else x
                    else:
                        x = jnp.where((lane & (tail - 1)) >= tail - d, 0.0, roll(mid, -d, 1))
                    buf[m, t, SUB:2 * SUB, :] = x
            for c in range(tiles):
                shifts = row_shifts(side)
                col_w = [nw[l, side, c, t] for t in range(SPAN)]
                row_w = [nw[l, side, c, SPAN + n] for n in range(len(shifts))]
                for g in range(2 if c < tiles - 1 else 1):
                    m = 2 * c + g
                    acc = None
                    for n, s in enumerate(shifts):
                        start = SUB + s if side == 0 else s
                        line = None
                        for t in range(SPAN):
                            term = col_w[t] * buf[m, t, pl.ds(start, SUB), :]
                            line = term if line is None else line + term
                        line = line * row_w[n]
                        acc = line if acc is None else acc + line
                    keep = sub < HALO if side == 0 else sub >= HALO
                    for h in range(2 if c < tiles - 1 else 4):
                        f = 2 * g + h if c < tiles - 1 else h
                        part = roll(acc, -tail, 1) if h >= 2 else acc
                        part = part if f % 2 == side else roll(part, HALO, 0)
                        part = jnp.where(keep, part, 0.0)
                        if c == 0:
                            spot = (f, l, c, pl.ds(base, SUB), slice(None))
                            ov[spot] = ov[spot] + part
                        else:
                            spot = (f, l, pl.ds(base, SUB), slice(c * LANES, c * LANES + widths[c]))
                            out[spot] = out[spot] + part[:, :widths[c]]
    columns(0)
    for copy in sends:
        copy.wait_send()


def solution(mesh):
    nband, nsector = mesh.shape["lat"], mesh.shape["lon"]

    def body(fields, dep_row, dep_col, weights):
        nf, nl, rows, cols = fields.shape
        tiles = pl.cdiv(cols, LANES)
        dims = (nf, nl, rows, cols, nband, nsector, cols * nsector)
        vmem = lambda *shape: pltpu.VMEM(shape, F32)
        groups = 2 * tiles - 1
        return pl.pallas_call(
            functools.partial(kernel, dims),
            out_shape=jax.ShapeDtypeStruct(fields.shape, F32),
            in_specs=[pl.BlockSpec(memory_space=pltpu.HBM)] * 4,
            out_specs=pl.BlockSpec(memory_space=pltpu.VMEM),
            scratch_shapes=[
                vmem(nf, nl, rows, cols),
                pltpu.VMEM((nl, rows, cols), jnp.int32),
                pltpu.VMEM((nl, rows, cols), jnp.int32),
                vmem(8, nl, rows, cols),
                vmem(nf, nl, tiles, rows, LANES),
                vmem(nl, tiles, 2 * SPAN, rows, LANES),
                vmem(tiles, nf, SPAN, rows + 2 * SUB, LANES),
                vmem(2, nl, groups, SUB, LANES), vmem(2, nl, groups, SUB, LANES),
                vmem(2, rows, LANES), vmem(2, rows, LANES),
                vmem(2, 2, SUB, LANES), vmem(2, 2, SUB, LANES),
                vmem(nl // PIECES, 2, groups, SPAN, 3 * SUB, LANES),
                vmem(nl, 2, tiles, SPAN + HALO, SUB, LANES),
                vmem(2, SPAN, rows + 2 * SUB, LANES),
                vmem(2, 2 * SPAN, rows, LANES),
                vmem(2, rows, LANES),
                pltpu.SemaphoreType.DMA((4,)),
                pltpu.SemaphoreType.DMA((6 + 2 * PIECES,)), pltpu.SemaphoreType.DMA((6 + 2 * PIECES,)),
            ],
            compiler_params=pltpu.CompilerParams(
                collective_id=0, has_side_effects=True, vmem_limit_bytes=40 << 20),
            name="advect",
        )(*[pltpu.with_memory_space_constraint(x, pltpu.HBM) for x in (fields, dep_row, dep_col, weights)])

    return jax.shard_map(
        body,
        mesh=mesh,
        in_specs=(
            P(None, None, "lat", "lon"),
            P(None, "lat", "lon"),
            P(None, "lat", "lon"),
            P(None, None, "lat", "lon"),
        ),
        out_specs=P(None, None, "lat", "lon"),
        check_vma=False,
    )
```
